32 devices in a mesh: row: 8 (over z, y), col: 4 (over x, core).
Axes of the slice: x: 2, y: 2, z: 4, core: 2. Of those that a mesh axis runs over, the one named last changes fastest.
Arguments:
- grams: bfloat16 [4, 3584, 3584], P(None, 'row', 'col'), as said below
- weights: bfloat16 [4, 3584, 7168], P(None, 'row', 'col'), may hold values from -6 to 6
Outputs:
- merged: float32 [3584, 7168], P('row', 'col')
- residual: float32 [3584, 7168], P('row', 'col')
The draws below stay inside these ranges and needn't reach their ends.
Inputs may be any that keep to these rules, and one draw needn't show every extreme that they name: `grams`: each of the 4 matrices is symmetric and positive definite.
All inputs are finite; a program needn't handle non-finite values.
Results may differ from the reference program's by a relative error of at most 0.012.
The reference program's roundings to bfloat16 on the way (of `rounded`) count: a program that leaves them out, or rounds other values in their place, can miss the bound.
Values may be sent and summed in bfloat16 or wider, within the bound.
A program may use at most 256 MiB of HBM per device.

```python
import math
import jax
import jax.numpy as jnp
from jax import lax

D = 3584
FF_COLS = 7168
MODELS = 4
ITERS = 2


def draw_grams(key, part):

    def one_model(model_key):
        scale_key, noise_key = jax.random.split(model_key)
        lowest, highest, spread = (0.5, 5.0, 0.3)
        scales = jnp.exp(jax.random.uniform(scale_key, (D,), jnp.float32, math.log(lowest), math.log(highest)))
        roots = jnp.sqrt(scales)
        noise = jax.random.normal(noise_key, (D, D), jnp.float32) * (spread / math.sqrt(D))
        core = jnp.eye(D, dtype=jnp.float32) + (noise + noise.T) * 0.5
        return (core * (roots[:, None] * roots[None, :])).astype(jnp.bfloat16)
    model_keys = jax.random.split(jax.random.fold_in(key, 17), MODELS)
    return jax.vmap(one_model)(model_keys)


def shard_levels(stream_key, shape, cuts, smallest, high):
    def one(position, parts):
        draws = jax.random.uniform(jax.random.fold_in(jax.random.fold_in(stream_key, 6), position), (parts,), jnp.float32, smallest / len(cuts), high / len(cuts))
        return jnp.repeat(jnp.exp(draws), shape[position] // parts).reshape((-1,) + (1,) * (len(shape) - position - 1))

    factor_of = one(*cuts[0])
    for cut in cuts[1:]:
        factor_of = factor_of * one(*cut)
    return factor_of


def bell_draw(rng, shape, width, limit, pieces=(), kind=jnp.bfloat16):
    factor_of = shard_levels(rng, shape, pieces, -0.22, 0.18) if pieces else 1.0
    values = jax.random.normal(rng, shape, jnp.float32) * width * factor_of
    return jnp.minimum(jnp.maximum(values, -limit), limit).astype(kind)


def setup_inputs(seed: int = 0) -> dict:
    streams_of = jax.random.split(jax.random.key(seed), 3)
    return {
        "grams": draw_grams(jax.random.fold_in(streams_of[2], 71), 0),
        "weights": bell_draw(streams_of[1], (MODELS, D, FF_COLS), 1.0, 6.0, ((1, 8), (2, 4))),
    }


def reference(grams, weights):
    high = lax.Precision.HIGHEST
    total = jnp.zeros((D, D), jnp.float32)
    right_side = jnp.zeros((D, FF_COLS), jnp.float32)
    for model_index in range(MODELS):
        gram_full = grams[model_index].astype(jnp.float32)
        weight = weights[model_index].astype(jnp.float32)
        gram_diag = jnp.diagonal(gram_full)
        right_side = right_side + 0.9 * jnp.dot(gram_full, weight, precision=high) + 0.1 * gram_diag[:, None] * weight
        total = total + gram_full
    total_diag = jnp.diagonal(total)
    merged = jnp.zeros((D, FF_COLS), jnp.float32)
    residual = right_side
    direction = right_side
    norm_now = jnp.sum(residual * residual, axis=0)
    for iteration in range(ITERS):
        rounded = lax.optimization_barrier(direction.astype(jnp.bfloat16)).astype(jnp.float32)
        mapped = 0.9 * jnp.dot(total, rounded, precision=high) + 0.1 * total_diag[:, None] * rounded
        curvature = jnp.sum(direction * mapped, axis=0)
        step_length = norm_now / curvature
        merged = merged + step_length * direction
        residual = residual - step_length * mapped
        if iteration + 1 < ITERS:
            norm_next = jnp.sum(residual * residual, axis=0)
            direction = residual + (norm_next / norm_now) * direction
            norm_now = norm_next
    return merged, residual
```

```python
import functools

import jax
import jax.numpy as jnp
from jax import lax
from jax.experimental import pallas as pl
from jax.experimental.pallas import tpu as pltpu
from jax.sharding import PartitionSpec as P

ITERS = 2
STREAMS = 2
MESH = pl.DeviceIdType.MESH


def ring_position(index, n):
    odd = index % 2
    return (1 - odd) * (index // 2) + odd * (n - 1 - index // 2)


def ring_index(position, n):
    back = position // (n // 2)
    return (1 - back) * 2 * position + back * (2 * (n - 1 - position) + 1)


def ring_product_kernel(n, x_ref, high_ref, low_ref, out_ref, ahead, behind, send_a, recv_a, send_b, recv_b):
    me = lax.axis_index("row")
    place = ring_position(me, n)
    right = ring_index((place + 1) % n, n)
    left = ring_index((place + n - 1) % n, n)
    half, columns = ahead.shape[2], x_ref.shape[1]

    barrier = pltpu.get_barrier_semaphore()
    for other in (left, right):
        pl.semaphore_signal(barrier, inc=1, device_id={"row": other}, device_id_type=MESH)
    pl.semaphore_wait(barrier, 2)

    def send(source, held, slot, sends, recvs, target):
        return pltpu.make_async_remote_copy(
            src_ref=source,
            dst_ref=held.at[slot],
            send_sem=sends.at[slot],
            recv_sem=recvs.at[slot],
            device_id={"row": target},
            device_id_type=MESH,
        )

    def add(where, owner, block):
        out_ref[:, where] += jnp.dot(high_ref[owner], block, preferred_element_type=jnp.float32) + jnp.dot(
            low_ref[owner], block, preferred_element_type=jnp.float32
        )

    front, rest = slice(0, half), slice(half, columns)
    send(x_ref.at[:, pl.ds(0, half)], ahead, 0, send_a, recv_a, right).start()
    send(x_ref.at[:, pl.ds(half, columns - half)], behind, 0, send_b, recv_b, left).start()
    out_ref[...] = jnp.zeros_like(out_ref)
    add(front, me, x_ref[:, front])
    add(rest, me, x_ref[:, rest])

    def step(s, carry):
        send(ahead.at[s], ahead, s, send_a, recv_a, right).wait()
        send(behind.at[s], behind, s, send_b, recv_b, left).wait()

        @pl.when(s < n - 2)
        def _():
            send(ahead.at[s], ahead, s + 1, send_a, recv_a, right).start()
            send(behind.at[s], behind, s + 1, send_b, recv_b, left).start()

        add(front, ring_index((place + n - 1 - s) % n, n), ahead[s])
        add(rest, ring_index((place + 1 + s) % n, n), behind[s])
        return carry

    lax.fori_loop(0, n - 1, step, 0)


def ring_product(n, rounded, high, low):
    rows, columns = rounded.shape
    half = pl.cdiv(columns, 256) * 128
    held = [pltpu.VMEM((n - 1, rows, size), jnp.bfloat16) for size in (half, columns - half)]
    return pl.pallas_call(
        functools.partial(ring_product_kernel, n),
        out_shape=jax.ShapeDtypeStruct((rows, columns), jnp.float32),
        in_specs=[pl.BlockSpec(memory_space=pltpu.VMEM)] * 3,
        out_specs=pl.BlockSpec(memory_space=pltpu.VMEM),
        scratch_shapes=held + [pltpu.SemaphoreType.DMA((n - 1,))] * 4,
        compiler_params=pltpu.CompilerParams(collective_id=1, has_side_effects=True, vmem_limit_bytes=48 * 2**20),
    )(rounded, high, low)


def row_sum_kernel(n, x_ref, out_ref, held, sends, recvs):
    me = lax.axis_index("row")
    barrier = pltpu.get_barrier_semaphore()
    for k in range(1, n):
        pl.semaphore_signal(barrier, inc=1, device_id={"row": (me + k) % n}, device_id_type=MESH)
    pl.semaphore_wait(barrier, n - 1)
    copies = []
    for k in range(1, n):
        copy = pltpu.make_async_remote_copy(
            src_ref=x_ref,
            dst_ref=held.at[k - 1],
            send_sem=sends.at[k - 1],
            recv_sem=recvs.at[k - 1],
            device_id={"row": (me + k) % n},
            device_id_type=MESH,
        )
        copy.start()
        copies.append(copy)
    for copy in copies:
        copy.wait()
    total = x_ref[...]
    for k in range(n - 1):
        total = total + held[k]
    out_ref[...] = total


def row_sum(n, values):
    flat = values.reshape(-1, 128)
    return pl.pallas_call(
        functools.partial(row_sum_kernel, n),
        out_shape=jax.ShapeDtypeStruct(flat.shape, jnp.float32),
        in_specs=[pl.BlockSpec(memory_space=pltpu.VMEM)],
        out_specs=pl.BlockSpec(memory_space=pltpu.VMEM),
        scratch_shapes=[pltpu.VMEM((n - 1,) + flat.shape, jnp.float32)] + [pltpu.SemaphoreType.DMA((n - 1,))] * 2,
        compiler_params=pltpu.CompilerParams(collective_id=2, has_side_effects=True),
    )(flat).reshape(values.shape)


def shards(row_count, grams, weights):
    models, slab_rows, slab_cols = grams.shape
    col_count = weights.shape[2]
    row_index = lax.axis_index("row")
    first_row = row_index * slab_rows
    width = col_count // STREAMS

    gathered = lax.all_gather(grams, "col", axis=0)
    parts = gathered.shape[0]

    def own_columns(array):
        per_slab = slab_cols // slab_rows
        slab = lax.dynamic_index_in_dim(array, row_index // per_slab, 0, keepdims=False)
        offset = (row_index % per_slab) * slab_rows
        return lax.dynamic_slice_in_dim(slab, offset, slab_rows, slab.ndim - 1)

    block = own_columns(gathered)
    on_diag = jnp.arange(slab_rows)[:, None] == jnp.arange(slab_rows)[None, :]
    diags = jnp.sum(jnp.where(on_diag, block.astype(jnp.float32), 0.0), axis=2)
    total_diag = jnp.sum(diags, axis=0)
    total = jnp.sum(gathered.astype(jnp.float32), axis=1)
    total = total.reshape(parts, slab_rows, -1, slab_rows).swapaxes(1, 2).reshape(row_count, slab_rows, slab_rows)
    high = total.astype(jnp.bfloat16)
    low = (total - high.astype(jnp.float32)).astype(jnp.bfloat16)
    first_part = (((0,), (0,)), ((), ()))
    depth = models * slab_rows
    flat = gathered.reshape(parts, depth, slab_cols)
    flat_block = block.reshape(depth, slab_rows)
    in_block = (jnp.arange(parts * slab_cols) // slab_rows) == row_index

    def right_side(weight):
        flat_weight = weight.reshape(depth, width)
        pieces = []
        for d in range(parts):
            piece = lax.dot_general(flat[d], flat_weight, first_part, preferred_element_type=jnp.float32)
            keep = in_block[d * slab_cols : (d + 1) * slab_cols]
            pieces.append(jnp.where(keep[:, None], 0.0, piece).astype(jnp.bfloat16))
        others = lax.psum_scatter(jnp.concatenate(pieces, axis=0), "row", scatter_dimension=0, tiled=True)
        own = lax.dot_general(flat_block, flat_weight, first_part, preferred_element_type=jnp.float32)
        diag_term = jnp.sum(diags[:, :, None] * weight.astype(jnp.float32), axis=0)
        return 0.9 * (own + others.astype(jnp.float32)) + 0.1 * diag_term

    def column_sum(values):
        return row_sum(row_count, jnp.sum(values, axis=0))

    starts = [right_side(lax.slice_in_dim(weights, s * width, (s + 1) * width, axis=2)) for s in range(STREAMS)]
    residual = jnp.concatenate(starts, axis=1)
    direction = residual
    merged = jnp.zeros_like(residual)
    norm_now = column_sum(residual * residual)
    for iteration in range(ITERS):
        rounded = direction.astype(jnp.bfloat16)
        product = ring_product(row_count, rounded, high, low)
        mapped = 0.9 * product + 0.1 * total_diag[:, None] * rounded.astype(jnp.float32)
        curvature = column_sum(direction * mapped)
        step_length = norm_now / curvature
        merged = merged + step_length * direction
        residual = residual - step_length * mapped
        if iteration + 1 < ITERS:
            norm_next = column_sum(residual * residual)
            direction = residual + norm_next / norm_now * direction
            norm_now = norm_next
    return merged, residual


def solution(mesh):
    placed = (P(None, "row", "col"), P(None, "row", "col"))
    return jax.shard_map(
        functools.partial(shards, mesh.shape["row"]),
        mesh=mesh,
        in_specs=placed,
        out_specs=(P("row", "col"), P("row", "col")),
        check_vma=False,
    )
```
